32 devices in a mesh: section: 8 (over z, y), tp: 4 (over x, core).
Axes of the slice: x: 2, y: 2, z: 4, core: 2. Of those that a mesh axis runs over, the one named last changes fastest.
Arguments:
- incoming: bfloat16 [8, 256, 6144], P('section', 'tp'), may hold values from -11 to 11, as said below
- grad_in: bfloat16 [8, 256, 6144], P('section', 'tp'), may hold values from -6 to 6
- held: bfloat16 [8, 2, 256, 6144], P('section', None, 'tp'), may hold values from -11 to 11, as said below
- roster: int32 [8, 2], replicated, may hold values from 0 to 1
- norm_gain: float32 [8, 6144], P('section'), may hold values from 0.25 to 1.75
- r_scores: float32 [8, 48, 256, 256], P('section', 'tp'), may hold values from -12 to 236
- value_weight: bfloat16 [8, 6144, 6144], P('section', None, 'tp'), may hold values from -0.078125 to 0.078125
- out_weight: bfloat16 [8, 6144, 6144], P('section', 'tp'), may hold values from -0.078125 to 0.078125
Outputs:
- act_out: bfloat16 [8, 256, 6144], P('section', 'tp')
- grad_out: bfloat16 [8, 256, 6144], P('section', 'tp')
- held_next: bfloat16 [8, 2, 256, 6144], P('section', None, 'tp')
The draws below stay inside these ranges and needn't reach their ends.
Inputs may be any that keep to these rules, and one draw needn't show every extreme that they name: `incoming`: every token row has its own scale. `held`: every token row has its own scale. roster[s, 0] names the slot at section 7 - s that holds section s's stash to fetch; roster[s, 1] names the slot there that takes section s's evicted input; the two may be equal.
All inputs are finite; a program needn't handle non-finite values.
Results may differ from the reference program's by a relative error of at most 0.0036.
Values may be sent and summed in bfloat16 or wider, within the bound.
A program may use at most 128 MiB of HBM per device.

```python
import math
import jax
import jax.numpy as jnp
from jax import lax

D = 6144
HEADS = 48
HEAD = 128
TOKENS = 256
SLOTS = 2
SECTIONS = 8


def scaled_rows(key, shape):
    first_key, second_key = jax.random.split(key)
    row_shape = shape[:-1] + (1,)
    base = jnp.clip(jax.random.normal(first_key, shape, jnp.float32), -5.5, 5.5)
    scales = jnp.exp(jax.random.uniform(second_key, row_shape, jnp.float32, math.log(0.25), math.log(2.0)))
    return base * scales


def draw_incoming(key, part):
    return scaled_rows(jax.random.fold_in(key, 11), (SECTIONS, TOKENS, D)).astype(jnp.bfloat16)


def draw_held(key, part):
    return scaled_rows(jax.random.fold_in(key, 12), (SECTIONS, SLOTS, TOKENS, D)).astype(jnp.bfloat16)


def draw_r_scores(key, part):
    first_key = jax.random.fold_in(jax.random.fold_in(key, 13), 0)
    shape = (SECTIONS, HEADS, TOKENS, TOKENS)
    return jnp.clip(2.0 * jax.random.normal(first_key, shape, jnp.float32), -12.0, 12.0)


def with_ends(result, rng, smallest, top_value):
    extent = result.shape
    index_at = [jax.random.randint(jax.random.fold_in(rng, axis), (), 0, extent[axis]) for axis in range(len(extent))]
    result = result.at[tuple(index_at)].set(smallest)
    longest = extent.index(max(extent))
    index_at[longest] = (index_at[longest] + 1) % extent[longest]
    return result.at[tuple(index_at)].set(top_value)


def block_scale(own_key, extent, shards, smallest, high):
    loudness = 1.0
    for dim, shards_of in shards:
        heights = jax.random.uniform(jax.random.fold_in(jax.random.fold_in(own_key, 6), dim), (shards_of,), jnp.float32, smallest / len(shards), high / len(shards))
        loudness = loudness * jnp.repeat(jnp.exp(heights), extent[dim] // shards_of).reshape((-1,) + (1,) * (len(extent) - 1 - dim))
    return loudness


def scatter_about(rng, dims, scale, reach, shards=(), kind=jnp.bfloat16):
    entries = jax.random.normal(rng, dims, jnp.float32) * scale
    if len(shards) > 0:
        entries = block_scale(rng, dims, shards, -0.22, 0.18) * entries
    return jnp.clip(entries, min=-reach, max=reach).astype(kind)


def setup_inputs(seed: int = 0) -> dict:
    streams_of = jax.random.split(jax.random.key(seed), 9)
    incoming = draw_incoming(jax.random.fold_in(streams_of[8], 71), 0)
    grad_in = scatter_about(streams_of[1], (SECTIONS, TOKENS, D), 1.0, 6.0, ((0, 8), (1, 4)))
    held = draw_held(jax.random.fold_in(streams_of[8], 71), 0)
    roster = with_ends(jax.random.randint(streams_of[3], (SECTIONS, 2), 0, SLOTS), jax.random.fold_in(streams_of[3], 1), 0, SLOTS - 1).astype(jnp.int32)
    norm_gain = jnp.clip(1.0 + 0.15 * jax.random.normal(streams_of[4], (SECTIONS, D), jnp.float32), 0.25, 1.75)
    r_scores = draw_r_scores(jax.random.fold_in(streams_of[8], 71), 0)
    value_weight = scatter_about(streams_of[6], (SECTIONS, D, HEADS * HEAD), D ** -0.5, 0.078125, ((0, 8), (2, 4)))
    out_weight = scatter_about(streams_of[7], (SECTIONS, HEADS * HEAD, D), (HEADS * HEAD) ** -0.5, 0.078125, ((0, 8), (1, 4)))
    return dict(incoming=incoming, grad_in=grad_in, held=held, roster=roster, norm_gain=norm_gain, r_scores=r_scores, value_weight=value_weight, out_weight=out_weight)


EPS = 0.5

def row_scale(values):
    return jnp.sqrt(lax.optimization_barrier(jnp.mean(values * values, axis=-1, keepdims=True)) + EPS)

def causal_probs(scores):
    length = scores.shape[-1]
    query_pos = jnp.arange(length)[:, None]
    key_pos = jnp.arange(length)[None, :]
    allowed = key_pos <= query_pos
    masked = jnp.where(allowed, scores, -jnp.inf)
    highest = lax.optimization_barrier(jnp.max(masked, axis=-1, keepdims=True))
    expo = jnp.where(allowed, jnp.exp(masked - highest), 0.0)
    return (expo / lax.optimization_barrier(jnp.sum(expo, axis=-1, keepdims=True))).astype(jnp.bfloat16)

def section_pass(operands):
    tokens_in, grad_rows, stash, gain, scores, w_value, w_out = operands
    length = tokens_in.shape[0]
    width = tokens_in.shape[1]
    heads = scores.shape[0]
    attn_probs = causal_probs(scores).astype(jnp.float32)
    tokens_f32 = tokens_in.astype(jnp.float32)
    normed = (tokens_f32 / row_scale(tokens_f32) * gain).astype(jnp.bfloat16)
    values = jnp.dot(normed, w_value, preferred_element_type=jnp.float32).astype(jnp.bfloat16)
    split_values = values.astype(jnp.float32).reshape(length, heads, -1)
    context = jnp.einsum('hij,jhd->ihd', attn_probs, split_values, precision=lax.Precision.HIGHEST)
    context = context.astype(jnp.bfloat16).reshape(length, -1)
    update = jnp.dot(context, w_out, preferred_element_type=jnp.float32)
    layer_out = (tokens_f32 + update).astype(jnp.bfloat16)
    grad_context = lax.dot_general(grad_rows, w_out, (((1,), (1,)), ((), ())), preferred_element_type=jnp.float32).astype(jnp.bfloat16)
    split_grad = grad_context.astype(jnp.float32).reshape(length, heads, -1)
    grad_values = jnp.einsum('hij,ihd->jhd', attn_probs, split_grad, precision=lax.Precision.HIGHEST)
    grad_values = grad_values.astype(jnp.bfloat16).reshape(length, -1)
    grad_normed = lax.dot_general(grad_values, w_value, (((1,), (1,)), ((), ())), preferred_element_type=jnp.float32)
    stash_f32 = stash.astype(jnp.float32)
    stash_scale = row_scale(stash_f32)
    inner_sum = lax.optimization_barrier(jnp.sum(gain * grad_normed * stash_f32, axis=-1, keepdims=True))
    input_grad = grad_rows.astype(jnp.float32) + gain * grad_normed / stash_scale - stash_f32 * inner_sum / (width * stash_scale ** 3)
    return (layer_out, input_grad.astype(jnp.bfloat16))

def reference(incoming, grad_in, held, roster, norm_gain, r_scores, value_weight, out_weight):
    count = incoming.shape[0]
    section_ids = jnp.arange(count).astype(jnp.int32)
    fetched = held[::-1][section_ids, roster[:, 0].astype(jnp.int32)]
    mirror_plan = roster[::-1]
    slot_ids = jnp.arange(held.shape[1]).astype(jnp.int32)
    chosen = slot_ids[None, :] == mirror_plan[:, 1][:, None]
    held_next = jnp.where(chosen[:, :, None, None], incoming[::-1][:, None], held)
    layer_out, input_grad = lax.map(section_pass, (incoming, grad_in, fetched, norm_gain, r_scores, value_weight, out_weight))
    return (jnp.roll(layer_out, 1, axis=0), jnp.roll(input_grad, -1, axis=0), held_next)
```

```python
import jax
import jax.numpy as jnp
from jax import lax
from jax.sharding import PartitionSpec as P


EPS = 0.5


CHUNKS = 2


def from_partner(value, bit):
    return lax.ppermute(value, "tp", [(i, i ^ 1 << bit) for i in range(lax.axis_size("tp"))])


def from_behind(block, distance):
    devices = range(lax.axis_size("section"))
    return lax.ppermute(block, "section", [((i - distance) % len(devices), i) for i in devices])


def from_mirror(block):
    devices = range(lax.axis_size("section"))
    return lax.ppermute(block, "section", [(len(devices) - 1 - i, i) for i in devices])


def tp_bits():
    return lax.axis_size("tp").bit_length() - 1


def own_bit(bit):
    return lax.axis_index("tp") >> bit & 1


def gather_rows(block):
    blocks = block
    for done, bit in enumerate(reversed(range(tp_bits()))):
        other = from_partner(blocks, bit)
        first = own_bit(bit) == 0
        blocks = jnp.stack(
            [jnp.where(first, blocks, other), jnp.where(first, other, blocks)], axis=done
        )
    return blocks.reshape(-1, block.shape[1])


def scatter_rows(partial):
    bits = tp_bits()
    part = partial.reshape((2,) * bits + (-1, partial.shape[1]))
    for bit in range(bits):
        at = bits - 1 - bit
        keep = lax.dynamic_index_in_dim(part, own_bit(bit), at, keepdims=False)
        give = lax.dynamic_index_in_dim(part, 1 - own_bit(bit), at, keepdims=False)
        got = from_partner(give.astype(jnp.bfloat16), bit)
        part = keep.astype(jnp.float32) + got.astype(jnp.float32)
    return part


def row_scale(values):
    return jnp.sqrt(jnp.mean(values * values, axis=-1, keepdims=True) + EPS)


def causal_probs(scores):
    length = scores.shape[-1]
    query_pos = lax.broadcasted_iota(jnp.int32, (length, length), 0)
    key_pos = lax.broadcasted_iota(jnp.int32, (length, length), 1)
    allowed = key_pos <= query_pos
    masked = jnp.where(allowed, scores, -jnp.inf)
    highest = jnp.max(masked, axis=-1, keepdims=True)
    expo = jnp.where(allowed, jnp.exp(masked - highest), 0.0)
    return (expo / jnp.sum(expo, axis=-1, keepdims=True)).astype(jnp.bfloat16)


def body(incoming, grad_in, held, roster, norm_gain, r_scores, value_weight, out_weight):
    tokens_here = incoming[0]
    grad_here = grad_in[0]
    stash_store = held[0]
    gain = norm_gain[0]
    w_value = value_weight[0]
    w_out = out_weight[0]
    heads_here = r_scores.shape[1]
    seq_len = r_scores.shape[2]
    width = tokens_here.shape[1]
    sections = lax.axis_size("section")
    mirror = sections - 1 - lax.axis_index("section")
    mirror_plan = lax.dynamic_index_in_dim(roster, mirror, 0, keepdims=False)

    tokens_f32 = tokens_here.astype(jnp.float32)
    normed = (tokens_f32 / row_scale(tokens_f32) * gain).astype(jnp.bfloat16)
    outgoing = lax.dynamic_index_in_dim(stash_store, mirror_plan[0], 0, keepdims=False)
    fetched = from_mirror(outgoing)
    arriving = from_mirror(tokens_here)
    all_grads = gather_rows(grad_here)
    all_normed = gather_rows(normed)
    fetched, _ = lax.optimization_barrier((fetched, all_normed))
    attn_probs = causal_probs(r_scores[0])

    grad_context = lax.dot_general(
        all_grads, w_out, (((1,), (1,)), ((), ())), preferred_element_type=jnp.float32
    ).astype(jnp.bfloat16)
    grad_values = jnp.einsum(
        "hij,ihd->jhd",
        attn_probs,
        grad_context.reshape(seq_len, heads_here, -1),
        preferred_element_type=jnp.float32,
    )
    grad_values = grad_values.astype(jnp.bfloat16).reshape(seq_len, -1)
    grad_normed = scatter_rows(
        lax.dot_general(
            grad_values, w_value, (((1,), (1,)), ((), ())), preferred_element_type=jnp.float32
        ),
    )
    stash_f32 = fetched.astype(jnp.float32)
    stash_scale = row_scale(stash_f32)
    inner_sum = jnp.sum(gain * grad_normed * stash_f32, axis=-1, keepdims=True)
    input_grad = (
        grad_here.astype(jnp.float32)
        + gain * grad_normed / stash_scale
        - stash_f32 * inner_sum / (width * stash_scale**3)
    )
    returned = from_behind(input_grad.astype(jnp.bfloat16), -1)

    values = jnp.dot(all_normed, w_value, preferred_element_type=jnp.float32)
    values = values.astype(jnp.bfloat16)
    context = jnp.einsum(
        "hij,jhd->ihd",
        attn_probs,
        values.reshape(seq_len, heads_here, -1),
        preferred_element_type=jnp.float32,
    )
    context = context.astype(jnp.bfloat16).reshape(seq_len, -1)
    passed_on = []
    span = width // CHUNKS
    for k in range(CHUNKS):
        columns = slice(k * span, (k + 1) * span)
        share = jnp.dot(context, w_out[:, columns], preferred_element_type=jnp.float32)
        update = scatter_rows(share)
        residual = tokens_here[:, columns]
        if k > 0:
            residual, layer_out = lax.optimization_barrier((residual, layer_out))
        layer_out = (residual.astype(jnp.float32) + update).astype(jnp.bfloat16)
        passed_on.append(from_behind(layer_out, 1))
    passed_on = jnp.concatenate(passed_on, axis=1)
    slot_match = jnp.arange(stash_store.shape[0]) == mirror_plan[1]
    held_next = jnp.where(slot_match[:, None, None], arriving[None], stash_store)
    return (passed_on[None], returned[None], held_next[None])


def solution(mesh):
    in_specs = (
        P("section", "tp", None),
        P("section", "tp", None),
        P("section", None, "tp", None),
        P(),
        P("section", None),
        P("section", "tp", None, None),
        P("section", None, "tp"),
        P("section", "tp", None),
    )
    out_specs = (P("section", "tp", None), P("section", "tp", None), P("section", None, "tp", None))
    return jax.shard_map(body, mesh=mesh, in_specs=in_specs, out_specs=out_specs, check_vma=False)
```

```python
import functools

import jax
import jax.numpy as jnp
from jax import lax
from jax.experimental import pallas as pl
from jax.experimental.pallas import tpu as pltpu
from jax.sharding import PartitionSpec as P


EPS = 0.5


CHUNKS = 2


def from_partner(value, bit):
    return lax.ppermute(value, "tp", [(i, i ^ 1 << bit) for i in range(lax.axis_size("tp"))])


def from_behind(block, distance):
    devices = range(lax.axis_size("section"))
    return lax.ppermute(block, "section", [((i - distance) % len(devices), i) for i in devices])


def from_mirror(block):
    devices = range(lax.axis_size("section"))
    return lax.ppermute(block, "section", [(len(devices) - 1 - i, i) for i in devices])


def tp_bits():
    return lax.axis_size("tp").bit_length() - 1


def gather_rows(block):
    blocks = block
    for done, bit in enumerate(reversed(range(tp_bits()))):
        other = from_partner(blocks, bit)
        blocks = jnp.stack([blocks, other], axis=done)
    return blocks.reshape(-1, block.shape[1])


def scatter_rows(partial):
    bits = tp_bits()
    part = partial.reshape((2,) * bits + (-1, partial.shape[1]))
    for bit in range(bits):
        at = bits - 1 - bit
        keep = lax.index_in_dim(part, 0, at, keepdims=False)
        give = lax.index_in_dim(part, 1, at, keepdims=False)
        got = from_partner(give.astype(jnp.bfloat16), bit)
        part = keep.astype(jnp.float32) + got.astype(jnp.float32)
    return part


def row_scale(values):
    return jnp.sqrt(jnp.mean(values * values, axis=-1, keepdims=True) + EPS)


def causal_probs(scores):
    length = scores.shape[-1]
    query_pos = lax.broadcasted_iota(jnp.int32, (length, length), 0)
    key_pos = lax.broadcasted_iota(jnp.int32, (length, length), 1)
    allowed = key_pos <= query_pos
    masked = jnp.where(allowed, scores, -jnp.inf)
    highest = jnp.max(masked, axis=-1, keepdims=True)
    expo = jnp.where(allowed, jnp.exp(masked - highest), 0.0)
    return (expo / jnp.sum(expo, axis=-1, keepdims=True)).astype(jnp.bfloat16)


def mix_kernel(blocks, over_queries, probs_ref, x_ref, out_ref, ordered, mixed):
    me = lax.axis_index("tp")
    rows = x_ref.shape[0] // blocks
    heads = probs_ref.shape[0]
    head = x_ref.shape[1] // heads
    for j in range(blocks):
        at = pl.ds(pl.multiple_of((me ^ j) * rows, rows), rows)
        ordered[at, :] = x_ref[j * rows : (j + 1) * rows, :]
    for h in range(heads):
        columns = slice(h * head, (h + 1) * head)
        mixed[:, columns] = lax.dot_general(
            probs_ref[h],
            ordered[:, columns],
            (((0 if over_queries else 1,), (0,)), ((), ())),
            preferred_element_type=jnp.float32,
        )
    for j in range(blocks):
        at = pl.ds(pl.multiple_of((me ^ j) * rows, rows), rows)
        out_ref[j * rows : (j + 1) * rows, :] = mixed[at, :].astype(out_ref.dtype)


def mix_tokens(probs, x, over_queries):
    heads, length, _ = probs.shape
    group = max(g for g in range(1, 5) if heads % g == 0)
    span = x.shape[1] // heads * group
    return pl.pallas_call(
        functools.partial(mix_kernel, lax.axis_size("tp"), over_queries),
        grid=(heads // group,),
        in_specs=[
            pl.BlockSpec((group, length, length), lambda i: (i, 0, 0)),
            pl.BlockSpec((length, span), lambda i: (0, i)),
        ],
        out_specs=pl.BlockSpec((length, span), lambda i: (0, i)),
        out_shape=jax.ShapeDtypeStruct(x.shape, jnp.bfloat16),
        scratch_shapes=[
            pltpu.VMEM((length, span), jnp.bfloat16),
            pltpu.VMEM((length, span), jnp.float32),
        ],
        compiler_params=pltpu.CompilerParams(vmem_limit_bytes=8 << 20),
        cost_estimate=pl.CostEstimate(
            flops=2 * length * length * x.shape[1],
            bytes_accessed=2 * probs.size + 4 * x.size,
            transcendentals=0,
        ),
    )(probs, x)


def body(incoming, grad_in, held, roster, norm_gain, r_scores, value_weight, out_weight):
    tokens_here = incoming[0]
    grad_here = grad_in[0]
    stash_store = held[0]
    gain = norm_gain[0]
    w_value = value_weight[0]
    w_out = out_weight[0]
    width = tokens_here.shape[1]
    sections = lax.axis_size("section")
    mirror = sections - 1 - lax.axis_index("section")
    mirror_plan = lax.dynamic_index_in_dim(roster, mirror, 0, keepdims=False)

    tokens_f32 = tokens_here.astype(jnp.float32)
    normed = (tokens_f32 / row_scale(tokens_f32) * gain).astype(jnp.bfloat16)
    outgoing = lax.dynamic_index_in_dim(stash_store, mirror_plan[0], 0, keepdims=False)
    fetched = from_mirror(outgoing)
    arriving = from_mirror(tokens_here)
    all_grads = gather_rows(grad_here)
    all_normed = gather_rows(normed)
    fetched, _ = lax.optimization_barrier((fetched, all_normed))
    attn_probs = causal_probs(r_scores[0])

    grad_context = lax.dot_general(
        all_grads, w_out, (((1,), (1,)), ((), ())), preferred_element_type=jnp.float32
    ).astype(jnp.bfloat16)
    grad_values = mix_tokens(attn_probs, grad_context, True)
    grad_normed = scatter_rows(
        lax.dot_general(
            grad_values, w_value, (((1,), (1,)), ((), ())), preferred_element_type=jnp.float32
        ),
    )
    stash_f32 = fetched.astype(jnp.float32)
    stash_scale = row_scale(stash_f32)
    inner_sum = jnp.sum(gain * grad_normed * stash_f32, axis=-1, keepdims=True)
    input_grad = (
        grad_here.astype(jnp.float32)
        + gain * grad_normed / stash_scale
        - stash_f32 * inner_sum / (width * stash_scale**3)
    )
    returned = from_behind(input_grad.astype(jnp.bfloat16), -1)

    values = jnp.dot(all_normed, w_value, preferred_element_type=jnp.float32)
    values = values.astype(jnp.bfloat16)
    context = mix_tokens(attn_probs, values, False)
    passed_on = []
    span = width // CHUNKS
    for k in range(CHUNKS):
        columns = slice(k * span, (k + 1) * span)
        share = jnp.dot(context, w_out[:, columns], preferred_element_type=jnp.float32)
        update = scatter_rows(share)
        residual = tokens_here[:, columns]
        if k > 0:
            residual, layer_out = lax.optimization_barrier((residual, layer_out))
        layer_out = (residual.astype(jnp.float32) + update).astype(jnp.bfloat16)
        passed_on.append(from_behind(layer_out, 1))
    passed_on = jnp.concatenate(passed_on, axis=1)
    slot_match = jnp.arange(stash_store.shape[0]) == mirror_plan[1]
    held_next = jnp.where(slot_match[:, None, None], arriving[None], stash_store)
    return (passed_on[None], returned[None], held_next[None])


def solution(mesh):
    in_specs = (
        P("section", "tp", None),
        P("section", "tp", None),
        P("section", None, "tp", None),
        P(),
        P("section", None),
        P("section", "tp", None, None),
        P("section", None, "tp"),
        P("section", "tp", None),
    )
    out_specs = (P("section", "tp", None), P("section", "tp", None), P("section", None, "tp", None))
    return jax.shard_map(body, mesh=mesh, in_specs=in_specs, out_specs=out_specs, check_vma=False)
```
